256 devices in a mesh: dp: 16 (over y, x_hi, core), mp: 16 (over z, x_lo).
Axes of the slice: x: 4 (x_hi: 2, x_lo: 2; x = x_hi * 2 + x_lo), y: 4, z: 8, core: 2. Of those that a mesh axis runs over, the one named last changes fastest.
Arguments:
- grad_parts: bfloat16 [16, 1, 6144, 6144], P('dp', None, None, 'mp'), may hold values from -6 to 6
- master: float32 [1, 6144, 6144], P(None, 'dp', 'mp'), may hold values from -6 to 6
- momentum: float32 [1, 6144, 6144], P(None, 'dp', 'mp'), may hold values from -4 to 4
Outputs:
- new_master: float32 [1, 6144, 6144], P(None, 'dp', 'mp')
- new_momentum: float32 [1, 6144, 6144], P(None, 'dp', 'mp')
- new_weights: bfloat16 [1, 6144, 6144], P(None, None, 'mp')
The draws below stay inside these ranges and needn't reach their ends.
All inputs are finite; a program needn't handle non-finite values.
Results may differ from the reference program's by a relative error of at most 0.0014.
Values may be sent and summed in bfloat16 or wider, within the bound.
A program may use at most 64 MiB of HBM per device.

```python
import jax
import jax.numpy as jnp
from jax import lax

D = 6144
LAYERS = 1
INNER = 6144
REPLICAS = 16


def spiked(drawn, rng, source, target, blocks, factor):
    owner, partner = [(jnp.arange(drawn.shape[axis_at]) // (drawn.shape[axis_at] // blocks)).reshape([-1 if axis == axis_at else 1 for axis in range(drawn.ndim)]) for axis_at in (source, target)]
    chosen = jax.random.permutation(rng, blocks)[partner]
    strong = (owner == chosen) | (owner == (partner + blocks // 2) % blocks)
    return jnp.where(strong, factor * drawn, drawn)


def levels(rng, dims, split, smallest, largest):
    factor_of = 1.0
    for axis_at, blocks in split:
        draws = jax.random.uniform(jax.random.fold_in(jax.random.fold_in(rng, 6), axis_at), (blocks,), jnp.float32, smallest / len(split), largest / len(split))
        factor_of = factor_of * jnp.repeat(jnp.exp(draws), dims[axis_at] // blocks).reshape((-1,) + (1,) * (len(dims) - 1 - axis_at))
    return factor_of


def bell_draw(own_key, extent, deviation, bound, cuts=(), held_as=jnp.bfloat16):
    values = deviation * jax.random.normal(own_key, extent, jnp.float32)
    if cuts:
        values = values * levels(own_key, extent, cuts, -0.22, 0.18)
    return jnp.clip(values, -bound, bound).astype(held_as)


def gaussian_with(stream_key, dims, spread, reach, shards, heavy, held_as=jnp.bfloat16):
    drawn = spread * jax.random.normal(stream_key, dims, jnp.float32)
    if shards:
        drawn = drawn * levels(stream_key, dims, shards, -0.22, 0.18)
    return jnp.clip(spiked(drawn, jax.random.fold_in(stream_key, 3), *heavy), -reach, reach).astype(held_as)


def setup_inputs(seed: int = 0) -> dict:
    seeds = jax.random.split(jax.random.key(seed), 4)
    grad_parts = gaussian_with(seeds[0], (REPLICAS, LAYERS, INNER, D), 1.0, 6.0, ((0, 16), (3, 16)), (0, 2, 16, 2.0))
    master = bell_draw(seeds[1], (LAYERS, INNER, D), 1.0, 6.0, ((1, 16), (2, 16)), jnp.float32)
    momentum = bell_draw(seeds[2], (LAYERS, INNER, D), 0.25, 4.0, ((1, 16), (2, 16)), jnp.float32)
    return dict(grad_parts=grad_parts, master=master, momentum=momentum)


beta_one = 0.9
beta_two = 0.99
step_size = 0.1
decay_rate = 0.1
softness = 0.05

def reference(grad_parts, master, momentum):
    gradient = lax.optimization_barrier(jnp.sum(grad_parts.astype(jnp.float32), axis=0)) / REPLICAS
    interp = beta_one * momentum + (1.0 - beta_one) * gradient
    direction = interp / jnp.sqrt(interp * interp + softness * softness)
    new_master = master - step_size * (direction + decay_rate * master)
    new_momentum = beta_two * momentum + (1.0 - beta_two) * gradient
    return (new_master, new_momentum, new_master.astype(jnp.bfloat16))
```

```python
import functools

import jax
import jax.numpy as jnp
from jax import lax
from jax.experimental import pallas as pl
from jax.experimental.pallas import tpu as pltpu
from jax.sharding import PartitionSpec as P

beta_one = 0.9
beta_two = 0.99
step_size = 0.1
decay_rate = 0.1
softness = 0.05

MESH = pl.DeviceIdType.MESH
A, B, X = 4, 2, 1

PIECES = ((0, 96, (A, X, B), (B, X, A)), (96, 96, (A, X, B), (B, X, A)), (192, 96, (A, X, B), (B, X, A)), (288, 96, (A, X, B), (B, X, A)))
LAG = 3.2


def reduce_slots(order, stage):
    taken = sum(order[:stage])
    slots = [s for s in range(8) if s & order[stage] and not s & taken]
    later = order[stage + 1 :]

    def urgency(s):
        hit = [i for i, d in enumerate(later) if s & d]
        return hit[0] if hit else len(later)

    return sorted(slots, key=urgency)


def tasks_of(piece, number):
    first, rows, down, up = piece
    start = number * LAG
    out = []
    for stage, at in ((0, 0.0), (1, 5.0), (2, 10.5)):
        for k, s in enumerate(reduce_slots(down, stage)):
            out.append((start + at + 0.2 * k, number, "reduce", stage, s))
    out.append((start + 13.5, number, "update", 0, 0))
    e1, e2, e3 = up
    for at, s in ((16.0, e1), (18.0, e2), (20.0, e1 + e2), (17.0, e3), (19.0, e1 + e3), (21.0, e2 + e3), (23.0, e1 + e2 + e3)):
        out.append((start + at, number, "spread", 0, s))
    return out


def kernel(
    grad, master, momentum, new_master, new_momentum, weights,
    own, part, outgoing, incoming, master_in, momentum_in,
    load_sem, pair_send, pair_recv, down_send, down_recv, up_send, up_recv, twin_send, twin_recv,
):
    dp, mp = lax.axis_index("dp"), lax.axis_index("mp")
    core, xh, y = lax.rem(dp, 2), lax.rem(dp // 2, 2), dp // 4
    side = 1 - 2 * lax.rem(y + core, 2)

    def device(y_at, x_at, c_at):
        return ((y_at * 2 + x_at) * 2 + c_at, mp)

    y_of = (y, lax.rem(y + 4 - side, 4), lax.rem(y + 4 + side, 4), lax.rem(y + 2, 4))
    x_of = (xh, 1 - xh)
    twin = device(y, xh, 1 - core)
    peer = {A: device(y_of[2], xh, core), B: device(y_of[1], xh, core), X: device(y, 1 - xh, core)}

    def tile_of(slot):
        return y_of[slot // 2], x_of[slot % 2]

    loads = [
        pltpu.make_async_copy(grad.at[:, :, core], own, load_sem.at[0]),
        pltpu.make_async_copy(master, master_in, load_sem.at[1]),
        pltpu.make_async_copy(momentum, momentum_in, load_sem.at[2]),
    ]
    for load in loads:
        load.start()

    barrier = pltpu.get_barrier_semaphore()
    for other in (twin, peer[A], peer[B], peer[X]):
        pl.semaphore_signal(barrier, inc=1, device_id=other, device_id_type=MESH)
    pl.semaphore_wait(barrier, 4)

    pairs = []
    for n, (first, rows, _, _) in enumerate(PIECES):
        at = pl.ds(first, rows)
        pairs.append(
            pltpu.make_async_remote_copy(
                src_ref=grad.at[:, :, 1 - core, at],
                dst_ref=part.at[:, :, at],
                send_sem=pair_send,
                recv_sem=pair_recv.at[n],
                device_id=twin,
                device_id_type=MESH,
            )
        )
        pairs[-1].start()
    loads[0].wait()

    def down_copy(n, slot, d):
        at = pl.ds(PIECES[n][0], PIECES[n][1])
        return pltpu.make_async_remote_copy(
            src_ref=outgoing.at[slot - 1, at],
            dst_ref=incoming.at[slot - 1, at],
            send_sem=down_send,
            recv_sem=down_recv.at[n * 7 + slot - 1],
            device_id=peer[d],
            device_id_type=MESH,
        )

    def up_copy(n, slot, d):
        at = pl.ds(PIECES[n][0], PIECES[n][1])
        ty, tx = tile_of(slot)
        here = weights.at[ty, tx, core, at]
        return pltpu.make_async_remote_copy(
            src_ref=here,
            dst_ref=here,
            send_sem=up_send,
            recv_sem=up_recv.at[n * 7 + (slot ^ d) - 1],
            device_id=peer[d],
            device_id_type=MESH,
        )

    def twin_copy(n, slot):
        at = pl.ds(PIECES[n][0], PIECES[n][1])
        ty, tx = tile_of(slot)
        here = weights.at[ty, tx, core, at]
        return pltpu.make_async_remote_copy(
            src_ref=here,
            dst_ref=here,
            send_sem=twin_send,
            recv_sem=twin_recv,
            device_id=twin,
            device_id_type=MESH,
        )

    def summed(n, slot, sources):
        at = pl.ds(PIECES[n][0], PIECES[n][1])
        ty, tx = tile_of(slot)
        total = own[ty, tx, at].astype(jnp.float32) + part[ty, tx, at].astype(jnp.float32)
        for source in sources:
            total += incoming[source - 1, at].astype(jnp.float32)
        return total

    begun, pair_in = set(), set()
    for _, n, kind, stage, slot in sorted(t for i, p in enumerate(PIECES) for t in tasks_of(p, i)):
        first, rows, down, up = PIECES[n]
        at = pl.ds(first, rows)
        if n not in pair_in:
            pairs[n].wait_recv()
            pair_in.add(n)
        if kind == "reduce":
            for d in down[:stage]:
                down_copy(n, slot | d, d).wait_recv()
            outgoing[slot - 1, at] = summed(n, slot, [slot | d for d in down[:stage]]).astype(jnp.bfloat16)
            down_copy(n, slot, down[stage]).start()
        elif kind == "update":
            if not begun:
                loads[1].wait()
                loads[2].wait()
                begun.add(n)
            for d in down:
                down_copy(n, d, d).wait_recv()
            gradient = summed(n, 0, down) / 16
            old_master, old_momentum = master_in[at], momentum_in[at]
            interp = beta_one * old_momentum + (1.0 - beta_one) * gradient
            direction = interp * lax.rsqrt(interp * interp + softness * softness)
            fresh = old_master - step_size * (direction + decay_rate * old_master)
            weights[y, xh, core, at] = fresh.astype(jnp.bfloat16)
            for d in up:
                up_copy(n, 0, d).start()
            twin_copy(n, 0).start()
            new_master[at] = fresh
            new_momentum[at] = beta_two * old_momentum + (1.0 - beta_two) * gradient
        else:
            last = max(i for i, d in enumerate(up) if slot & d)
            up_copy(n, slot ^ up[last], up[last]).wait_recv()
            for d in up[last + 1 :]:
                up_copy(n, slot, d).start()
            twin_copy(n, slot).start()

    pltpu.make_async_copy(own, own, twin_recv).wait()
    pltpu.make_async_copy(own, own, twin_send).wait()
    pltpu.make_async_copy(own, own, pair_send).wait()
    pltpu.make_async_copy(outgoing, outgoing, down_send).wait()
    pltpu.make_async_copy(outgoing, outgoing, up_send).wait()


def per_device(grad_parts, master, momentum):
    side, columns = master.shape[1:]
    grad = grad_parts.reshape(4, 2, 2, side, columns)
    pieces = len(PIECES)
    new_master, new_momentum, weights = pl.pallas_call(
        kernel,
        out_shape=(
            jax.ShapeDtypeStruct((side, columns), jnp.float32),
            jax.ShapeDtypeStruct((side, columns), jnp.float32),
            jax.ShapeDtypeStruct((4, 2, 2, side, columns), jnp.bfloat16),
        ),
        in_specs=[pl.BlockSpec(memory_space=pl.ANY)] * 3,
        out_specs=[pl.BlockSpec(memory_space=pltpu.VMEM)] * 3,
        scratch_shapes=[
            pltpu.VMEM((4, 2, side, columns), jnp.bfloat16),
            pltpu.VMEM((4, 2, side, columns), jnp.bfloat16),
            pltpu.VMEM((7, side, columns), jnp.bfloat16),
            pltpu.VMEM((7, side, columns), jnp.bfloat16),
            pltpu.VMEM((side, columns), jnp.float32),
            pltpu.VMEM((side, columns), jnp.float32),
            pltpu.SemaphoreType.DMA((3,)),
            pltpu.SemaphoreType.DMA,
            pltpu.SemaphoreType.DMA((pieces,)),
            pltpu.SemaphoreType.DMA,
            pltpu.SemaphoreType.DMA((7 * pieces,)),
            pltpu.SemaphoreType.DMA,
            pltpu.SemaphoreType.DMA((7 * pieces,)),
            pltpu.SemaphoreType.DMA,
            pltpu.SemaphoreType.DMA,
        ],
        compiler_params=pltpu.CompilerParams(collective_id=0, has_side_effects=True, vmem_limit_bytes=48 * 2**20),
    )(grad, master.reshape(side, columns), momentum.reshape(side, columns))
    return (
        new_master.reshape(1, side, columns),
        new_momentum.reshape(1, side, columns),
        weights.reshape(1, 16 * side, columns),
    )


def solution(mesh):
    return jax.shard_map(
        per_device,
        mesh=mesh,
        in_specs=(P("dp", None, None, "mp"), P(None, "dp", "mp"), P(None, "dp", "mp")),
        out_specs=(P(None, "dp", "mp"), P(None, "dp", "mp"), P(None, None, "mp")),
        check_vma=False,
    )
```

```python
import functools

import jax
import jax.numpy as jnp
from jax import lax
from jax.experimental import pallas as pl
from jax.experimental.pallas import tpu as pltpu
from jax.sharding import PartitionSpec as P

beta_one = 0.9
beta_two = 0.99
step_size = 0.1
decay_rate = 0.1
softness = 0.05

MESH = pl.DeviceIdType.MESH
A, B, X = 4, 2, 1

PIECES = (
    (0, 16, (A, B, X), (B, A, X)),
    (16, 32, (X, B, A), (A, B, X)),
    (48, 32, (B, A, X), (B, X, A)),
    (80, 64, (B, A, X), (X, B, A)),
    (144, 80, (X, A, B), (A, B, X)),
    (224, 48, (B, A, X), (B, X, A)),
    (272, 64, (B, A, X), (X, B, A)),
    (336, 48, (X, A, B), (X, B, A)),
)
STEPS = (
    6, 7, 5, 4, 19, 23, 21, 17, 38, 39, 35, 34, 54, 55, 51, 50, 69, 71, 67, 65,
    86, 87, 83, 82, 102, 103, 99, 98, 2, 3, 117, 119, 115, 113, 36, 37, 18, 22, 52, 53,
    68, 84, 33, 85, 70, 49, 100, 101, 116, 118, 81, 66, 1, 40, 20, 97, 56, 114, 88, 72,
    44, 8, 42, 24, 41, 60, 58, 104, 92, 120, 57, 90, 76, 89, 12, 46, 74, 10, 28, 73,
    9, 26, 45, 43, 25, 106, 62, 122, 105, 108, 121, 59, 124, 91, 61, 78, 94, 30, 77, 93,
    13, 14, 47, 107, 75, 110, 11, 123, 126, 29, 109, 27, 125, 63, 95, 79, 111, 31, 127, 15,
)


def kernel(
    grad, master, momentum, new_master, new_momentum, weights,
    own, part, outgoing, incoming, master_in, momentum_in,
    load_sem, pair_send, pair_recv, down_send, down_recv, up_send, up_recv, twin_send, twin_recv,
):
    dp, mp = lax.axis_index("dp"), lax.axis_index("mp")
    core, xh, y = lax.rem(dp, 2), lax.rem(dp // 2, 2), dp // 4
    side = 1 - 2 * lax.rem(y + core, 2)

    def device(y_at, x_at, c_at):
        return ((y_at * 2 + x_at) * 2 + c_at, mp)

    y_of = (y, lax.rem(y + 4 - side, 4), lax.rem(y + 4 + side, 4), lax.rem(y + 2, 4))
    x_of = (xh, 1 - xh)
    twin = device(y, xh, 1 - core)
    peer = {A: device(y_of[2], xh, core), B: device(y_of[1], xh, core), X: device(y, 1 - xh, core)}

    def tile_of(slot):
        return y_of[slot // 2], x_of[slot % 2]

    loads = [
        pltpu.make_async_copy(grad.at[:, :, core], own, load_sem.at[0]),
        pltpu.make_async_copy(master, master_in, load_sem.at[1]),
        pltpu.make_async_copy(momentum, momentum_in, load_sem.at[2]),
    ]
    for load in loads:
        load.start()

    barrier = pltpu.get_barrier_semaphore()
    for other in (twin, peer[A], peer[B], peer[X]):
        pl.semaphore_signal(barrier, inc=1, device_id=other, device_id_type=MESH)
    pl.semaphore_wait(barrier, 4)

    pairs = []
    for n, (first, rows, _, _) in enumerate(PIECES):
        at = pl.ds(first, rows)
        pairs.append(
            pltpu.make_async_remote_copy(
                src_ref=grad.at[:, :, 1 - core, at],
                dst_ref=part.at[:, :, at],
                send_sem=pair_send,
                recv_sem=pair_recv.at[n],
                device_id=twin,
                device_id_type=MESH,
            )
        )
        pairs[-1].start()
    loads[0].wait()

    def down_copy(n, slot, d):
        at = pl.ds(PIECES[n][0], PIECES[n][1])
        return pltpu.make_async_remote_copy(
            src_ref=outgoing.at[slot - 1, at],
            dst_ref=incoming.at[slot - 1, at],
            send_sem=down_send,
            recv_sem=down_recv.at[n * 7 + slot - 1],
            device_id=peer[d],
            device_id_type=MESH,
        )

    def up_copy(n, slot, d):
        at = pl.ds(PIECES[n][0], PIECES[n][1])
        ty, tx = tile_of(slot)
        here = weights.at[ty, tx, core, at]
        return pltpu.make_async_remote_copy(
            src_ref=here,
            dst_ref=here,
            send_sem=up_send,
            recv_sem=up_recv.at[n * 7 + (slot ^ d) - 1],
            device_id=peer[d],
            device_id_type=MESH,
        )

    def twin_copy(n, slot):
        at = pl.ds(PIECES[n][0], PIECES[n][1])
        ty, tx = tile_of(slot)
        here = weights.at[ty, tx, core, at]
        return pltpu.make_async_remote_copy(
            src_ref=here,
            dst_ref=here,
            send_sem=twin_send,
            recv_sem=twin_recv,
            device_id=twin,
            device_id_type=MESH,
        )

    def summed(n, slot, sources):
        at = pl.ds(PIECES[n][0], PIECES[n][1])
        ty, tx = tile_of(slot)
        total = own[ty, tx, at].astype(jnp.float32) + part[ty, tx, at].astype(jnp.float32)
        for source in sources:
            total += incoming[source - 1, at].astype(jnp.float32)
        return total

    ready, paired = False, set()
    for step in STEPS:
        n, slot = step // 16, step % 8
        first, rows, down, up = PIECES[n]
        at = pl.ds(first, rows)
        if n not in paired:
            pairs[n].wait_recv()
            paired.add(n)
        if step % 16 >= 8 and slot:
            last = max(i for i, d in enumerate(up) if slot & d)
            up_copy(n, slot ^ up[last], up[last]).wait_recv()
            for d in up[last + 1 :]:
                up_copy(n, slot, d).start()
            twin_copy(n, slot).start()
        elif slot:
            stage = min(i for i, d in enumerate(down) if slot & d)
            for d in down[:stage]:
                down_copy(n, slot | d, d).wait_recv()
            outgoing[slot - 1, at] = summed(n, slot, [slot | d for d in down[:stage]]).astype(jnp.bfloat16)
            down_copy(n, slot, down[stage]).start()
        else:
            if not ready:
                loads[1].wait()
                loads[2].wait()
                ready = True
            for d in down:
                down_copy(n, d, d).wait_recv()
            gradient = summed(n, 0, down) / 16
            old_master, old_momentum = master_in[at], momentum_in[at]
            interp = beta_one * old_momentum + (1.0 - beta_one) * gradient
            direction = interp * lax.rsqrt(interp * interp + softness * softness)
            fresh = old_master - step_size * (direction + decay_rate * old_master)
            weights[y, xh, core, at] = fresh.astype(jnp.bfloat16)
            for d in up:
                up_copy(n, 0, d).start()
            twin_copy(n, 0).start()
            new_master[at] = fresh
            new_momentum[at] = beta_two * old_momentum + (1.0 - beta_two) * gradient

    pltpu.make_async_copy(own, own, twin_recv).wait()
    pltpu.make_async_copy(own, own, twin_send).wait()
    pltpu.make_async_copy(own, own, pair_send).wait()
    pltpu.make_async_copy(outgoing, outgoing, down_send).wait()
    pltpu.make_async_copy(outgoing, outgoing, up_send).wait()


def put_out(fresh, moved, rounded, new_master, new_momentum, weights, sem):
    copies = [
        pltpu.make_async_copy(fresh, new_master, sem.at[0]),
        pltpu.make_async_copy(moved, new_momentum, sem.at[1]),
    ]
    for n in range(4):
        copies.append(pltpu.make_async_copy(rounded.at[n], weights.at[n], sem.at[2 + n]))
    for copy in copies:
        copy.start()
    for copy in copies:
        copy.wait()


def per_device(grad_parts, master, momentum):
    side, columns = master.shape[1:]
    grad = grad_parts.reshape(4, 2, 2, side, columns)
    pieces = len(PIECES)
    outs = (((side, columns), jnp.float32), ((side, columns), jnp.float32), ((4, 2, 2, side, columns), jnp.bfloat16))
    results = pl.pallas_call(
        kernel,
        out_shape=[pltpu.VMEM(*o) for o in outs],
        in_specs=[pl.BlockSpec(memory_space=pltpu.HBM)] * 3,
        out_specs=[pl.BlockSpec(memory_space=pltpu.VMEM)] * 3,
        scratch_shapes=[
            pltpu.VMEM((4, 2, side, columns), jnp.bfloat16),
            pltpu.VMEM((4, 2, side, columns), jnp.bfloat16),
            pltpu.VMEM((7, side, columns), jnp.bfloat16),
            pltpu.VMEM((7, side, columns), jnp.bfloat16),
            pltpu.VMEM((side, columns), jnp.float32),
            pltpu.VMEM((side, columns), jnp.float32),
            pltpu.SemaphoreType.DMA((3,)),
            pltpu.SemaphoreType.DMA,
            pltpu.SemaphoreType.DMA((pieces,)),
            pltpu.SemaphoreType.DMA,
            pltpu.SemaphoreType.DMA((7 * pieces,)),
            pltpu.SemaphoreType.DMA,
            pltpu.SemaphoreType.DMA((7 * pieces,)),
            pltpu.SemaphoreType.DMA,
            pltpu.SemaphoreType.DMA,
        ],
        compiler_params=pltpu.CompilerParams(collective_id=0, has_side_effects=True, vmem_limit_bytes=48 * 2**20),
    )(grad, master.reshape(side, columns), momentum.reshape(side, columns))
    new_master, new_momentum, weights = pl.pallas_call(
        put_out,
        out_shape=[jax.ShapeDtypeStruct(*o) for o in outs],
        in_specs=[pl.BlockSpec(memory_space=pltpu.VMEM)] * 3,
        out_specs=[pl.BlockSpec(memory_space=pltpu.HBM)] * 3,
        scratch_shapes=[pltpu.SemaphoreType.DMA((6,))],
        compiler_params=pltpu.CompilerParams(vmem_limit_bytes=2**20),
    )(*[pltpu.with_memory_space_constraint(r, pltpu.VMEM) for r in results])
    return (
        new_master.reshape(1, side, columns),
        new_momentum.reshape(1, side, columns),
        weights.reshape(1, 16 * side, columns),
    )


def solution(mesh):
    return jax.shard_map(
        per_device,
        mesh=mesh,
        in_specs=(P("dp", None, None, "mp"), P(None, "dp", "mp"), P(None, "dp", "mp")),
        out_specs=(P(None, "dp", "mp"), P(None, "dp", "mp"), P(None, None, "mp")),
        check_vma=False,
    )
```

```python
import functools

import jax
import jax.numpy as jnp
from jax import lax
from jax.experimental import pallas as pl
from jax.experimental.pallas import tpu as pltpu
from jax.sharding import PartitionSpec as P

beta_one = 0.9
beta_two = 0.99
step_size = 0.1
decay_rate = 0.1
softness = 0.05

MESH = pl.DeviceIdType.MESH
A, B, X = 4, 2, 1

PIECES = (
    (0, 32, (B, A, X), (A, X, B)),
    (32, 32, (X, A, B), (A, X, B)),
    (64, 32, (X, A, B), (X, A, B)),
    (96, 48, (A, X, B), (X, A, B)),
    (144, 64, (B, A, X), (B, A, X)),
    (208, 32, (B, A, X), (A, B, X)),
    (240, 48, (X, A, B), (B, A, X)),
    (288, 48, (X, B, A), (X, A, B)),
    (336, 48, (B, A, X), (X, A, B)),
)
EARLY = 64
STEPS = (
    7, 21, 23, 2, 3, 19, 71, 55, 103, 86, 52, 82, 135, 39, 67, 54, 134, 101, 87, 37,
    35, 119, 5, 99, 53, 69, 6, 33, 117, 51, 70, 131, 102, 115, 22, 133, 36, 1, 38, 84,
    65, 118, 83, 98, 66, 85, 130, 49, 113, 68, 129, 50, 4, 100, 81, 116, 20, 17, 114, 34,
    132, 18, 97, 72, 56, 8, 120, 24, 88, 136, 104, 12, 40, 121, 74, 25, 92, 28, 60, 57,
    106, 137, 108, 13, 94, 9, 140, 76, 124, 78, 41, 110, 75, 125, 30, 29, 141, 44, 61, 90,
    93, 45, 123, 127, 43, 59, 31, 14, 79, 15, 107, 139, 111, 63, 95, 143, 47,
)


def parse(step):
    n, slot = step // 16, step % 8
    return n, slot, "up" if step % 16 > 8 else "down"


def arrival_of(n, way, slot):
    up = PIECES[n][3]
    return (n, way, slot | up[0] if way == "up" and slot & up[2] else slot)


def stage_of(order, slot):
    return min((i for i, d in enumerate(order) if slot & d), default=3)


def tiles_of(n, slot):
    up = PIECES[n][3]
    return [slot ^ up[0], slot] if slot & up[2] else [slot]


def beyond(n, slot):
    up = PIECES[n][3]
    return up[max(i for i, d in enumerate(up) if slot & d) + 1 :]


def messages_of(step):
    n, slot, way = parse(step)
    down, up = PIECES[n][2:]
    if way == "up":
        return [(d, arrival_of(n, way, s | d)) for s in tiles_of(n, slot) for d in beyond(n, s)]
    if slot:
        d = down[stage_of(down, slot)]
        return [(d, (n, way, slot ^ d))]
    return [(d, arrival_of(n, "up", d)) for d in up]


def numbered():
    first, sent = {}, {}
    for at, step in enumerate(STEPS):
        n, slot, way = parse(step)
        halves = () if way == "up" else (0,) if stage_of(PIECES[n][2], slot) == 0 else (0, 1)
        for key in [(n, way, slot)] + [(n, "pair", half) for half in halves]:
            first.setdefault(key, at)
        for d, key in messages_of(step):
            sent.setdefault(key, []).append((d, at))
    links = [(d, at, first[key]) for key in sent for d, at in sent[key]]
    number, last = {}, []
    for n in range(len(PIECES)):
        for half in range(2):
            number[n, "pair", half] = len(last)
            last.append(first[n, "pair", half])
    for key in sorted(sent, key=lambda k: min(at for _, at in sent[k])):
        fit = [
            (then, i)
            for i, then in enumerate(last)
            if all(any(d == e and then <= v and r <= at for e, v, r in links) for d, at in sent[key])
        ]
        i = max(fit)[1] if fit else len(last)
        if not fit:
            last.append(0)
        number[key], last[i] = i, first[key]
    return number, len(last)


NUMBER, SEMAPHORES = numbered()


def kernel(
    grad, master, momentum, new_master, new_momentum, weights,
    own, other, part, outgoing, incoming, master_in, momentum_in,
    load_sem, recv_sem, pair_send, down_send, up_send, twin_send, twin_recv,
):
    dp, mp = lax.axis_index("dp"), lax.axis_index("mp")
    core, xh, y = lax.rem(dp, 2), lax.rem(dp // 2, 2), dp // 4
    side = 1 - 2 * lax.rem(y + core, 2)

    def device(y_at, x_at, c_at):
        return ((y_at * 2 + x_at) * 2 + c_at, mp)

    y_of = (y, lax.rem(y + 4 - side, 4), lax.rem(y + 4 + side, 4), lax.rem(y + 2, 4))
    x_of = (xh, 1 - xh)
    twin = device(y, xh, 1 - core)
    peer = {A: device(y_of[2], xh, core), B: device(y_of[1], xh, core), X: device(y, 1 - xh, core)}

    def tile_of(slot):
        return y_of[slot // 2], x_of[slot % 2]

    def rows_of(n):
        return pl.ds(PIECES[n][0], PIECES[n][1])

    def send(source, target, send_sem, recv_sem, to):
        pltpu.make_async_remote_copy(
            src_ref=source, dst_ref=target, send_sem=send_sem, recv_sem=recv_sem, device_id=to, device_id_type=MESH
        ).start()

    def await_bytes(ref, sem):
        pltpu.make_async_copy(ref, ref, sem).wait()

    barrier = pltpu.get_barrier_semaphore()
    for neighbour in (twin, peer[A], peer[B], peer[X]):
        pl.semaphore_signal(barrier, inc=1, device_id=neighbour, device_id_type=MESH)

    loads = []
    for start, stop in ((0, EARLY), (EARLY, own.shape[2])):
        at = pl.ds(start, stop - start)
        for of, to in ((1 - core, other), (core, own)):
            loads.append(pltpu.make_async_copy(grad.at[:, :, of, at], to.at[:, :, at], load_sem.at[len(loads)]))
    loads.append(pltpu.make_async_copy(master, master_in, load_sem.at[4]))
    loads.append(pltpu.make_async_copy(momentum, momentum_in, load_sem.at[5]))
    for load in loads:
        load.start()
    there = set()

    def need(key, wait):
        if key not in there:
            wait()
            there.add(key)

    pl.semaphore_wait(barrier, 4)

    for half in range(2):
        for n, (first, rows, down, _) in enumerate(PIECES):
            load = 0 if first < EARLY else 2
            need(("load", load), loads[load].wait)
            at = rows_of(n)
            if down[0] == X:
                spots = [(slice(None), x_of[1 - half])]
            elif down[0] == A:
                spots = [(y_of[k], slice(None)) for k in ((1, 3), (0, 2))[half]]
            else:
                spots = [(y_of[k], slice(None)) for k in ((2, 3), (0, 1))[half]]
            for ty, tx in spots:
                send(other.at[ty, tx, at], part.at[ty, tx, at], pair_send, recv_sem.at[NUMBER[n, "pair", half]], twin)

    def pass_up(n, slot, along):
        ty, tx = tile_of(slot)
        here = weights.at[ty, tx, core, rows_of(n)]
        for d in along:
            send(here, here, up_send, recv_sem.at[NUMBER[arrival_of(n, "up", slot | d)]], peer[d])
        send(here, here, twin_send, twin_recv, twin)

    def summed(n, slot, sources):
        at = rows_of(n)
        if sources:
            await_bytes(incoming.at[pl.ds(0, len(sources)), at], recv_sem.at[NUMBER[n, "down", slot]])
        ty, tx = tile_of(slot)
        total = own[ty, tx, at].astype(jnp.float32) + part[ty, tx, at].astype(jnp.float32)
        for source in sources:
            total += incoming[source - 1, at].astype(jnp.float32)
        return total

    for step in STEPS:
        n, slot, way = parse(step)
        first, rows, down, up = PIECES[n]
        at = rows_of(n)
        if way == "up":
            tiles = tiles_of(n, slot)
            await_bytes(incoming.at[pl.ds(0, len(tiles)), at], recv_sem.at[NUMBER[n, way, slot]])
            for tile in tiles:
                pass_up(n, tile, beyond(n, tile))
            continue
        load = 1 if first < EARLY else 3
        need(("load", load), loads[load].wait)
        stage = stage_of(down, slot)
        for half in range(2 if stage else 1):
            need(("part", n, half), lambda: await_bytes(part.at[:, 0, at], recv_sem.at[NUMBER[n, "pair", half]]))
        if slot:
            outgoing[slot - 1, at] = summed(n, slot, [slot | d for d in down[:stage]]).astype(jnp.bfloat16)
            d = down[stage]
            key = (n, way, slot ^ d)
            send(outgoing.at[slot - 1, at], incoming.at[slot - 1, at], down_send, recv_sem.at[NUMBER[key]], peer[d])
        else:
            need(("load", 4), loads[4].wait)
            need(("load", 5), loads[5].wait)
            gradient = summed(n, 0, down) / 16
            old_master, old_momentum = master_in[at], momentum_in[at]
            interp = beta_one * old_momentum + (1.0 - beta_one) * gradient
            direction = interp * lax.rsqrt(interp * interp + softness * softness)
            fresh = old_master - step_size * (direction + decay_rate * old_master)
            weights[y, xh, core, at] = fresh.astype(jnp.bfloat16)
            pass_up(n, 0, up)
            new_master[at] = fresh
            new_momentum[at] = beta_two * old_momentum + (1.0 - beta_two) * gradient

    for sem in (twin_recv, twin_send, pair_send):
        await_bytes(own, sem)
    for sem in (down_send, up_send):
        await_bytes(outgoing, sem)


def put_out(fresh, moved, rounded, new_master, new_momentum, weights, sem):
    copies = [
        pltpu.make_async_copy(fresh, new_master, sem.at[0]),
        pltpu.make_async_copy(moved, new_momentum, sem.at[1]),
    ]
    for n in range(4):
        copies.append(pltpu.make_async_copy(rounded.at[n], weights.at[n], sem.at[2 + n]))
    for copy in copies:
        copy.start()
    for copy in copies:
        copy.wait()


def per_device(grad_parts, master, momentum):
    side, columns = master.shape[1:]
    grad = grad_parts.reshape(4, 2, 2, side, columns)
    outs = (((side, columns), jnp.float32), ((side, columns), jnp.float32), ((4, 2, 2, side, columns), jnp.bfloat16))
    results = pl.pallas_call(
        kernel,
        out_shape=[pltpu.VMEM(*o) for o in outs],
        in_specs=[pl.BlockSpec(memory_space=pltpu.HBM)] * 3,
        out_specs=[pl.BlockSpec(memory_space=pltpu.VMEM)] * 3,
        scratch_shapes=[
            pltpu.VMEM((4, 2, side, columns), jnp.bfloat16),
            pltpu.VMEM((4, 2, side, columns), jnp.bfloat16),
            pltpu.VMEM((4, 2, side, columns), jnp.bfloat16),
            pltpu.VMEM((7, side, columns), jnp.bfloat16),
            pltpu.VMEM((7, side, columns), jnp.bfloat16),
            pltpu.VMEM((side, columns), jnp.float32),
            pltpu.VMEM((side, columns), jnp.float32),
            pltpu.SemaphoreType.DMA((6,)),
            pltpu.SemaphoreType.DMA((SEMAPHORES,)),
            pltpu.SemaphoreType.DMA,
            pltpu.SemaphoreType.DMA,
            pltpu.SemaphoreType.DMA,
            pltpu.SemaphoreType.DMA,
            pltpu.SemaphoreType.DMA,
        ],
        compiler_params=pltpu.CompilerParams(collective_id=0, has_side_effects=True, vmem_limit_bytes=48 * 2**20),
    )(grad, master.reshape(side, columns), momentum.reshape(side, columns))
    new_master, new_momentum, weights = pl.pallas_call(
        put_out,
        out_shape=[jax.ShapeDtypeStruct(*o) for o in outs],
        in_specs=[pl.BlockSpec(memory_space=pltpu.VMEM)] * 3,
        out_specs=[pl.BlockSpec(memory_space=pltpu.HBM)] * 3,
        scratch_shapes=[pltpu.SemaphoreType.DMA((6,))],
        compiler_params=pltpu.CompilerParams(vmem_limit_bytes=2**20),
    )(*[pltpu.with_memory_space_constraint(r, pltpu.VMEM) for r in results])
    return (
        new_master.reshape(1, side, columns),
        new_momentum.reshape(1, side, columns),
        weights.reshape(1, 16 * side, columns),
    )


def solution(mesh):
    return jax.shard_map(
        per_device,
        mesh=mesh,
        in_specs=(P("dp", None, None, "mp"), P(None, "dp", "mp"), P(None, "dp", "mp")),
        out_specs=(P(None, "dp", "mp"), P(None, "dp", "mp"), P(None, None, "mp")),
        check_vma=False,
    )
```

```python
import functools

import jax
import jax.numpy as jnp
from jax import lax
from jax.experimental import pallas as pl
from jax.experimental.pallas import tpu as pltpu
from jax.sharding import PartitionSpec as P

beta_one = 0.9
beta_two = 0.99
step_size = 0.1
decay_rate = 0.1
softness = 0.05

MESH = pl.DeviceIdType.MESH
A, B, X = 4, 2, 1

PIECES = (
    (0, 32, (B, A, X), (B, X, A)),
    (32, 80, (X, A, B), (B, X, A)),
    (112, 16, (B, A, X), (A, B, X)),
    (128, 32, (A, X, B), (B, X, A)),
    (160, 48, (X, B, A), (X, B, A)),
    (208, 32, (X, A, B), (X, B, A)),
    (240, 48, (A, B, X), (X, A, B)),
    (288, 48, (B, A, X), (A, B, X)),
    (336, 32, (B, A, X), (A, B, X)),
    (368, 16, (A, B, X), (A, B, X)),
)
EARLY = 112
STEPS = (
    7, 2, 3, 6, 23, 53, 54, 115, 102, 55, 151, 119, 67, 103, 135, 134, 100, 87, 69, 85,
    5, 71, 17, 83, 39, 150, 19, 101, 149, 148, 130, 114, 131, 38, 147, 99, 22, 98, 21, 86,
    1, 52, 133, 35, 146, 70, 37, 36, 51, 145, 132, 65, 118, 4, 34, 117, 18, 97, 49, 84,
    33, 81, 129, 66, 20, 82, 68, 50, 8, 113, 116, 152, 104, 24, 56, 40, 72, 120, 10, 88,
    154, 136, 58, 44, 156, 105, 26, 9, 73, 42, 124, 140, 138, 89, 108, 158, 122, 25, 46, 107,
    57, 74, 14, 45, 59, 75, 11, 109, 126, 27, 62, 77, 142, 90, 91, 47, 111, 159, 93, 141,
    79, 125, 15, 157, 63, 127, 31, 30, 143, 95,
)


def parse(step):
    n, slot = step // 16, step % 8
    return n, slot, "up" if step % 16 > 8 else "down"


def arrival_of(n, way, slot):
    up = PIECES[n][3]
    return (n, way, slot | up[0] if way == "up" and slot & up[2] else slot)


def stage_of(order, slot):
    return min((i for i, d in enumerate(order) if slot & d), default=3)


def tiles_of(n, slot):
    up = PIECES[n][3]
    return [slot ^ up[0], slot] if slot & up[2] else [slot]


def beyond(n, slot):
    up = PIECES[n][3]
    return up[max(i for i, d in enumerate(up) if slot & d) + 1 :]


def messages_of(step):
    n, slot, way = parse(step)
    down, up = PIECES[n][2:]
    if way == "up":
        return [(d, arrival_of(n, way, s | d)) for s in tiles_of(n, slot) for d in beyond(n, s)]
    if slot:
        d = down[stage_of(down, slot)]
        return [(d, (n, way, slot ^ d))]
    return [(d, arrival_of(n, "up", d)) for d in up]


def numbered():
    first, sent = {}, {}
    for at, step in enumerate(STEPS):
        n, slot, way = parse(step)
        halves = () if way == "up" else (0,) if stage_of(PIECES[n][2], slot) == 0 else (0, 1)
        for key in [(n, way, slot)] + [(n * (1 - half), "pair", half) for half in halves]:
            first.setdefault(key, at)
        for d, key in messages_of(step):
            sent.setdefault(key, []).append((d, at))
    links = [(d, at, first[key]) for key in sent for d, at in sent[key]]
    number, last = {}, []
    for n, half in [(n, 0) for n in range(len(PIECES))] + [(0, 1)]:
        number[n, "pair", half] = len(last)
        last.append(first[n, "pair", half])
    for key in sorted(sent, key=lambda k: min(at for _, at in sent[k])):
        fit = [
            (then, i)
            for i, then in enumerate(last)
            if all(any(d == e and then <= v and r <= at for e, v, r in links) for d, at in sent[key])
        ]
        i = max(fit)[1] if fit else len(last)
        if not fit:
            last.append(0)
        number[key], last[i] = i, first[key]
    return number, len(last)


NUMBER, SEMAPHORES = numbered()


def kernel(
    grad, master, momentum, new_master, new_momentum, weights,
    own, other, part, outgoing, incoming, master_in, momentum_in,
    load_sem, recv_sem, pair_send, down_send, up_send, twin_send, twin_recv,
):
    dp, mp = lax.axis_index("dp"), lax.axis_index("mp")
    core, xh, y = lax.rem(dp, 2), lax.rem(dp // 2, 2), dp // 4
    side = 1 - 2 * lax.rem(y + core, 2)

    def device(y_at, x_at, c_at):
        return ((y_at * 2 + x_at) * 2 + c_at, mp)

    y_of = (y, lax.rem(y + 4 - side, 4), lax.rem(y + 4 + side, 4), lax.rem(y + 2, 4))
    x_of = (xh, 1 - xh)
    twin = device(y, xh, 1 - core)
    peer = {A: device(y_of[2], xh, core), B: device(y_of[1], xh, core), X: device(y, 1 - xh, core)}

    def tile_of(slot):
        return y_of[slot // 2], x_of[slot % 2]

    def rows_of(n):
        return pl.ds(PIECES[n][0], PIECES[n][1])

    def send(source, target, send_sem, recv_sem, to):
        pltpu.make_async_remote_copy(
            src_ref=source, dst_ref=target, send_sem=send_sem, recv_sem=recv_sem, device_id=to, device_id_type=MESH
        ).start()

    def await_bytes(ref, sem):
        pltpu.make_async_copy(ref, ref, sem).wait()

    barrier = pltpu.get_barrier_semaphore()
    for neighbour in (twin, peer[A], peer[B], peer[X]):
        pl.semaphore_signal(barrier, inc=1, device_id=neighbour, device_id_type=MESH)

    loads = []
    for start, stop in ((0, EARLY), (EARLY, own.shape[2])):
        at = pl.ds(start, stop - start)
        for of, to in ((1 - core, other), (core, own)):
            loads.append(pltpu.make_async_copy(grad.at[:, :, of, at], to.at[:, :, at], load_sem.at[len(loads)]))
    loads.append(pltpu.make_async_copy(master, master_in, load_sem.at[4]))
    loads.append(pltpu.make_async_copy(momentum, momentum_in, load_sem.at[5]))
    for load in loads:
        load.start()
    there = set()

    def need(key, wait):
        if key not in there:
            wait()
            there.add(key)

    pl.semaphore_wait(barrier, 4)

    for half in range(2):
        for n, (first, rows, down, _) in enumerate(PIECES):
            load = 0 if first < EARLY else 2
            need(("load", load), loads[load].wait)
            at = rows_of(n)
            if down[0] == X:
                spots = [(slice(None), x_of[1 - half])]
            elif down[0] == A:
                spots = [(y_of[k], slice(None)) for k in ((1, 3), (0, 2))[half]]
            else:
                spots = [(y_of[k], slice(None)) for k in ((2, 3), (0, 1))[half]]
            for ty, tx in spots:
                send(other.at[ty, tx, at], part.at[ty, tx, at], pair_send, recv_sem.at[NUMBER[n * (1 - half), "pair", half]], twin)

    def pass_up(n, slot, along):
        ty, tx = tile_of(slot)
        here = weights.at[ty, tx, core, rows_of(n)]
        for d in along:
            send(here, here, up_send, recv_sem.at[NUMBER[arrival_of(n, "up", slot | d)]], peer[d])
        send(here, here, twin_send, twin_recv, twin)

    def summed(n, slot, sources):
        at = rows_of(n)
        if sources:
            await_bytes(incoming.at[pl.ds(0, len(sources)), at], recv_sem.at[NUMBER[n, "down", slot]])
        ty, tx = tile_of(slot)
        total = own[ty, tx, at].astype(jnp.float32) + part[ty, tx, at].astype(jnp.float32)
        for source in sources:
            total += incoming[source - 1, at].astype(jnp.float32)
        return total

    for step in STEPS:
        n, slot, way = parse(step)
        first, rows, down, up = PIECES[n]
        at = rows_of(n)
        if way == "up":
            tiles = tiles_of(n, slot)
            await_bytes(incoming.at[pl.ds(0, len(tiles)), at], recv_sem.at[NUMBER[n, way, slot]])
            for tile in tiles:
                pass_up(n, tile, beyond(n, tile))
            continue
        load = 1 if first < EARLY else 3
        need(("load", load), loads[load].wait)
        stage = stage_of(down, slot)
        need(("part", n), lambda: await_bytes(part.at[:, 0, at], recv_sem.at[NUMBER[n, "pair", 0]]))
        if stage:
            need("part", lambda: await_bytes(part.at[:, 0], recv_sem.at[NUMBER[0, "pair", 1]]))
        if slot:
            outgoing[slot - 1, at] = summed(n, slot, [slot | d for d in down[:stage]]).astype(jnp.bfloat16)
            d = down[stage]
            key = (n, way, slot ^ d)
            send(outgoing.at[slot - 1, at], incoming.at[slot - 1, at], down_send, recv_sem.at[NUMBER[key]], peer[d])
        else:
            need(("load", 4), loads[4].wait)
            need(("load", 5), loads[5].wait)
            gradient = summed(n, 0, down) / 16
            old_master, old_momentum = master_in[at], momentum_in[at]
            interp = beta_one * old_momentum + (1.0 - beta_one) * gradient
            direction = interp * lax.rsqrt(interp * interp + softness * softness)
            fresh = old_master - step_size * (direction + decay_rate * old_master)
            weights[y, xh, core, at] = fresh.astype(jnp.bfloat16)
            pass_up(n, 0, up)
            new_master[at] = fresh
            new_momentum[at] = beta_two * old_momentum + (1.0 - beta_two) * gradient

    for sem in (twin_recv, twin_send, pair_send):
        await_bytes(own, sem)
    for sem in (down_send, up_send):
        await_bytes(outgoing, sem)


def put_out(fresh, moved, rounded, new_master, new_momentum, weights, sem):
    copies = [
        pltpu.make_async_copy(fresh, new_master, sem.at[0]),
        pltpu.make_async_copy(moved, new_momentum, sem.at[1]),
    ]
    for n in range(4):
        copies.append(pltpu.make_async_copy(rounded.at[n], weights.at[n], sem.at[2 + n]))
    for copy in copies:
        copy.start()
    for copy in copies:
        copy.wait()


def per_device(grad_parts, master, momentum):
    side, columns = master.shape[1:]
    grad = grad_parts.reshape(4, 2, 2, side, columns)
    outs = (((side, columns), jnp.float32), ((side, columns), jnp.float32), ((4, 2, 2, side, columns), jnp.bfloat16))
    results = pl.pallas_call(
        kernel,
        out_shape=[pltpu.VMEM(*o) for o in outs],
        in_specs=[pl.BlockSpec(memory_space=pltpu.HBM)] * 3,
        out_specs=[pl.BlockSpec(memory_space=pltpu.VMEM)] * 3,
        scratch_shapes=[
            pltpu.VMEM((4, 2, side, columns), jnp.bfloat16),
            pltpu.VMEM((4, 2, side, columns), jnp.bfloat16),
            pltpu.VMEM((4, 2, side, columns), jnp.bfloat16),
            pltpu.VMEM((7, side, columns), jnp.bfloat16),
            pltpu.VMEM((7, side, columns), jnp.bfloat16),
            pltpu.VMEM((side, columns), jnp.float32),
            pltpu.VMEM((side, columns), jnp.float32),
            pltpu.SemaphoreType.DMA((6,)),
            pltpu.SemaphoreType.DMA((SEMAPHORES,)),
            pltpu.SemaphoreType.DMA,
            pltpu.SemaphoreType.DMA,
            pltpu.SemaphoreType.DMA,
            pltpu.SemaphoreType.DMA,
            pltpu.SemaphoreType.DMA,
        ],
        compiler_params=pltpu.CompilerParams(collective_id=0, has_side_effects=True, vmem_limit_bytes=48 * 2**20),
    )(grad, master.reshape(side, columns), momentum.reshape(side, columns))
    new_master, new_momentum, weights = pl.pallas_call(
        put_out,
        out_shape=[jax.ShapeDtypeStruct(*o) for o in outs],
        in_specs=[pl.BlockSpec(memory_space=pltpu.VMEM)] * 3,
        out_specs=[pl.BlockSpec(memory_space=pltpu.HBM)] * 3,
        scratch_shapes=[pltpu.SemaphoreType.DMA((6,))],
        compiler_params=pltpu.CompilerParams(vmem_limit_bytes=2**20),
    )(*[pltpu.with_memory_space_constraint(r, pltpu.VMEM) for r in results])
    return (
        new_master.reshape(1, side, columns),
        new_momentum.reshape(1, side, columns),
        weights.reshape(1, 16 * side, columns),
    )


def solution(mesh):
    return jax.shard_map(
        per_device,
        mesh=mesh,
        in_specs=(P("dp", None, None, "mp"), P(None, "dp", "mp"), P(None, "dp", "mp")),
        out_specs=(P(None, "dp", "mp"), P(None, "dp", "mp"), P(None, None, "mp")),
        check_vma=False,
    )
```

```python
import functools

import jax
import jax.numpy as jnp
from jax import lax
from jax.experimental import pallas as pl
from jax.experimental.pallas import tpu as pltpu
from jax.sharding import PartitionSpec as P

beta_one = 0.9
beta_two = 0.99
step_size = 0.1
decay_rate = 0.1
softness = 0.05

MESH = pl.DeviceIdType.MESH
A, B, X = 4, 2, 1

PIECES = (
    (0, 32, (B, A, X), (B, X, A)),
    (32, 80, (X, A, B), (B, X, A)),
    (112, 16, (B, A, X), (A, B, X)),
    (128, 32, (A, X, B), (B, X, A)),
    (160, 48, (X, B, A), (X, B, A)),
    (208, 32, (X, A, B), (X, B, A)),
    (240, 48, (A, B, X), (X, A, B)),
    (288, 48, (B, A, X), (A, B, X)),
    (336, 32, (B, A, X), (A, B, X)),
    (368, 16, (A, B, X), (A, B, X)),
)
EARLY = 112
STEPS = (
    7, 2, 3, 6, 23, 53, 54, 115, 102, 55, 151, 119, 67, 103, 135, 134, 100, 87, 69, 85,
    5, 71, 17, 83, 39, 150, 19, 101, 149, 148, 130, 114, 131, 38, 147, 99, 22, 98, 21, 86,
    1, 52, 133, 35, 146, 70, 37, 36, 51, 145, 132, 65, 118, 4, 34, 117, 18, 97, 49, 84,
    33, 81, 129, 66, 20, 82, 68, 50, 8, 113, 116, 152, 104, 24, 56, 40, 72, 120, 10, 88,
    154, 136, 58, 44, 156, 105, 26, 9, 73, 42, 124, 140, 138, 89, 108, 158, 122, 25, 46, 107,
    57, 74, 14, 45, 59, 75, 11, 109, 126, 27, 62, 77, 142, 90, 91, 47, 111, 159, 93, 141,
    79, 125, 15, 157, 63, 127, 31, 30, 143, 95,
)


def parse(step):
    n, slot = step // 16, step % 8
    return n, slot, "up" if step % 16 > 8 else "down"


def arrival_of(n, way, slot):
    up = PIECES[n][3]
    return (n, way, slot | up[0] if way == "up" and slot & up[2] else slot)


def stage_of(order, slot):
    return min((i for i, d in enumerate(order) if slot & d), default=3)


def tiles_of(n, slot):
    up = PIECES[n][3]
    return [slot ^ up[0], slot] if slot & up[2] else [slot]


def beyond(n, slot):
    up = PIECES[n][3]
    return up[max(i for i, d in enumerate(up) if slot & d) + 1 :]


def messages_of(step):
    n, slot, way = parse(step)
    down, up = PIECES[n][2:]
    if way == "up":
        return [(d, arrival_of(n, way, s | d)) for s in tiles_of(n, slot) for d in beyond(n, s)]
    if slot:
        d = down[stage_of(down, slot)]
        return [(d, (n, way, slot ^ d))]
    return [(d, arrival_of(n, "up", d)) for d in up]


def numbered():
    first, sent = {}, {}
    for at, step in enumerate(STEPS):
        n, slot, way = parse(step)
        halves = () if way == "up" else (0,) if stage_of(PIECES[n][2], slot) == 0 else (0, 1)
        for key in [(n, way, slot)] + [(n * (1 - half), "pair", half) for half in halves]:
            first.setdefault(key, at)
        for d, key in messages_of(step):
            sent.setdefault(key, []).append((d, at))
    links = [(d, at, first[key]) for key in sent for d, at in sent[key]]
    number, last = {}, []
    for n, half in [(n, 0) for n in range(len(PIECES))] + [(0, 1)]:
        number[n, "pair", half] = len(last)
        last.append(first[n, "pair", half])
    for key in sorted(sent, key=lambda k: min(at for _, at in sent[k])):
        fit = [
            (then, i)
            for i, then in enumerate(last)
            if all(any(d == e and then <= v and r <= at for e, v, r in links) for d, at in sent[key])
        ]
        i = max(fit)[1] if fit else len(last)
        if not fit:
            last.append(0)
        number[key], last[i] = i, first[key]
    return number, len(last)


NUMBER, SEMAPHORES = numbered()


def kernel(
    grad, master, momentum, new_master, new_momentum, weights,
    own, other, part, outgoing, incoming, master_in, momentum_in,
    load_sem, recv_sem, pair_send, down_send, up_send, twin_send, twin_recv,
):
    dp, mp = lax.axis_index("dp"), lax.axis_index("mp")
    core, xh, y = lax.rem(dp, 2), lax.rem(dp // 2, 2), dp // 4
    side = 1 - 2 * lax.rem(y + core, 2)

    def device(y_at, x_at, c_at):
        return ((y_at * 2 + x_at) * 2 + c_at, mp)

    y_of = (y, lax.rem(y + 4 - side, 4), lax.rem(y + 4 + side, 4), lax.rem(y + 2, 4))
    x_of = (xh, 1 - xh)
    twin = device(y, xh, 1 - core)
    peer = {A: device(y_of[2], xh, core), B: device(y_of[1], xh, core), X: device(y, 1 - xh, core)}

    def tile_of(slot):
        return y_of[slot // 2], x_of[slot % 2]

    def rows_of(n):
        return pl.ds(PIECES[n][0], PIECES[n][1])

    def send(source, target, send_sem, recv_sem, to):
        pltpu.make_async_remote_copy(
            src_ref=source, dst_ref=target, send_sem=send_sem, recv_sem=recv_sem, device_id=to, device_id_type=MESH
        ).start()

    def await_bytes(ref, sem):
        pltpu.make_async_copy(ref, ref, sem).wait()

    barrier = pltpu.get_barrier_semaphore()
    for neighbour in (twin, peer[A], peer[B], peer[X]):
        pl.semaphore_signal(barrier, inc=1, device_id=neighbour, device_id_type=MESH)

    loads = []
    for start, stop in ((0, EARLY), (EARLY, own.shape[2])):
        at = pl.ds(start, stop - start)
        for of, to in ((1 - core, other), (core, own)):
            loads.append(pltpu.make_async_copy(grad.at[:, :, of, at], to.at[:, :, at], load_sem.at[len(loads)]))
    loads.append(pltpu.make_async_copy(master, master_in, load_sem.at[4]))
    loads.append(pltpu.make_async_copy(momentum, momentum_in, load_sem.at[5]))
    for load in loads[:4]:
        load.start()
    there = set()

    def need(key, wait):
        if key not in there:
            wait()
            there.add(key)

    pl.semaphore_wait(barrier, 4)

    for half in range(2):
        for n, (first, rows, down, _) in enumerate(PIECES):
            load = 0 if first < EARLY else 2
            need(("load", load), loads[load].wait)
            at = rows_of(n)
            if down[0] == X:
                spots = [(slice(None), x_of[1 - half])]
            elif down[0] == A:
                spots = [(y_of[k], slice(None)) for k in ((1, 3), (0, 2))[half]]
            else:
                spots = [(y_of[k], slice(None)) for k in ((2, 3), (0, 1))[half]]
            for ty, tx in spots:
                send(other.at[ty, tx, at], part.at[ty, tx, at], pair_send, recv_sem.at[NUMBER[n * (1 - half), "pair", half]], twin)

    for load in loads[4:]:
        load.start()

    def pass_up(n, slot, along):
        ty, tx = tile_of(slot)
        here = weights.at[ty, tx, core, rows_of(n)]
        for d in along:
            send(here, here, up_send, recv_sem.at[NUMBER[arrival_of(n, "up", slot | d)]], peer[d])
        send(here, here, twin_send, twin_recv, twin)

    def summed(n, slot, sources):
        at = rows_of(n)
        if sources:
            await_bytes(incoming.at[pl.ds(0, len(sources)), at], recv_sem.at[NUMBER[n, "down", slot]])
        ty, tx = tile_of(slot)
        total = own[ty, tx, at].astype(jnp.float32) + part[ty, tx, at].astype(jnp.float32)
        for source in sources:
            total += incoming[source - 1, at].astype(jnp.float32)
        return total

    for step in STEPS:
        n, slot, way = parse(step)
        first, rows, down, up = PIECES[n]
        at = rows_of(n)
        if way == "up":
            tiles = tiles_of(n, slot)
            await_bytes(incoming.at[pl.ds(0, len(tiles)), at], recv_sem.at[NUMBER[n, way, slot]])
            for tile in tiles:
                pass_up(n, tile, beyond(n, tile))
            continue
        load = 1 if first < EARLY else 3
        need(("load", load), loads[load].wait)
        stage = stage_of(down, slot)
        need(("part", n), lambda: await_bytes(part.at[:, 0, at], recv_sem.at[NUMBER[n, "pair", 0]]))
        if stage:
            need("part", lambda: await_bytes(part.at[:, 0], recv_sem.at[NUMBER[0, "pair", 1]]))
        if slot:
            outgoing[slot - 1, at] = summed(n, slot, [slot | d for d in down[:stage]]).astype(jnp.bfloat16)
            d = down[stage]
            key = (n, way, slot ^ d)
            send(outgoing.at[slot - 1, at], incoming.at[slot - 1, at], down_send, recv_sem.at[NUMBER[key]], peer[d])
        else:
            need(("load", 4), loads[4].wait)
            need(("load", 5), loads[5].wait)
            gradient = summed(n, 0, down) / 16
            old_master, old_momentum = master_in[at], momentum_in[at]
            interp = beta_one * old_momentum + (1.0 - beta_one) * gradient
            direction = interp * lax.rsqrt(interp * interp + softness * softness)
            fresh = old_master - step_size * (direction + decay_rate * old_master)
            weights[y, xh, core, at] = fresh.astype(jnp.bfloat16)
            pass_up(n, 0, up)
            new_master[at] = fresh
            new_momentum[at] = beta_two * old_momentum + (1.0 - beta_two) * gradient

    for sem in (twin_recv, twin_send, pair_send):
        await_bytes(own, sem)
    for sem in (down_send, up_send):
        await_bytes(outgoing, sem)


def put_out(fresh, moved, rounded, new_master, new_momentum, weights, sem):
    copies = [
        pltpu.make_async_copy(fresh, new_master, sem.at[0]),
        pltpu.make_async_copy(moved, new_momentum, sem.at[1]),
    ]
    for n in range(4):
        copies.append(pltpu.make_async_copy(rounded.at[n], weights.at[n], sem.at[2 + n]))
    for copy in copies:
        copy.start()
    for copy in copies:
        copy.wait()


def per_device(grad_parts, master, momentum):
    side, columns = master.shape[1:]
    grad = grad_parts.reshape(4, 2, 2, side, columns)
    outs = (((side, columns), jnp.float32), ((side, columns), jnp.float32), ((4, 2, 2, side, columns), jnp.bfloat16))
    results = pl.pallas_call(
        kernel,
        out_shape=[pltpu.VMEM(*o) for o in outs],
        in_specs=[pl.BlockSpec(memory_space=pltpu.HBM)] * 3,
        out_specs=[pl.BlockSpec(memory_space=pltpu.VMEM)] * 3,
        scratch_shapes=[
            pltpu.VMEM((4, 2, side, columns), jnp.bfloat16),
            pltpu.VMEM((4, 2, side, columns), jnp.bfloat16),
            pltpu.VMEM((4, 2, side, columns), jnp.bfloat16),
            pltpu.VMEM((7, side, columns), jnp.bfloat16),
            pltpu.VMEM((7, side, columns), jnp.bfloat16),
            pltpu.VMEM((side, columns), jnp.float32),
            pltpu.VMEM((side, columns), jnp.float32),
            pltpu.SemaphoreType.DMA((6,)),
            pltpu.SemaphoreType.DMA((SEMAPHORES,)),
            pltpu.SemaphoreType.DMA,
            pltpu.SemaphoreType.DMA,
            pltpu.SemaphoreType.DMA,
            pltpu.SemaphoreType.DMA,
            pltpu.SemaphoreType.DMA,
        ],
        compiler_params=pltpu.CompilerParams(collective_id=0, has_side_effects=True, vmem_limit_bytes=48 * 2**20),
    )(grad, master.reshape(side, columns), momentum.reshape(side, columns))
    new_master, new_momentum, weights = pl.pallas_call(
        put_out,
        out_shape=[jax.ShapeDtypeStruct(*o) for o in outs],
        in_specs=[pl.BlockSpec(memory_space=pltpu.VMEM)] * 3,
        out_specs=[pl.BlockSpec(memory_space=pltpu.HBM)] * 3,
        scratch_shapes=[pltpu.SemaphoreType.DMA((6,))],
        compiler_params=pltpu.CompilerParams(vmem_limit_bytes=2**20),
    )(*[pltpu.with_memory_space_constraint(r, pltpu.VMEM) for r in results])
    return (
        new_master.reshape(1, side, columns),
        new_momentum.reshape(1, side, columns),
        weights.reshape(1, 16 * side, columns),
    )


def solution(mesh):
    return jax.shard_map(
        per_device,
        mesh=mesh,
        in_specs=(P("dp", None, None, "mp"), P(None, "dp", "mp"), P(None, "dp", "mp")),
        out_specs=(P(None, "dp", "mp"), P(None, "dp", "mp"), P(None, None, "mp")),
        check_vma=False,
    )
```
